64 devices in a mesh: dp: 4 (over x, y), cp: 16 (over z, core).
Axes of the slice: x: 2, y: 2, z: 8, core: 2. Of those that a mesh axis runs over, the one named last changes fastest.
The devices are a block of a 4x4x8 slice.
Arguments:
- q_rope: bfloat16 [4, 8192, 40, 128], P('dp', 'cp'), parts along dimension 0
- k_rope: bfloat16 [4, 8192, 8, 128], P('dp', 'cp'), parts along dimension 0
- values: bfloat16 [4, 8192, 8, 128], P('dp', 'cp'), parts along dimension 0
- d_out: bfloat16 [4, 8192, 40, 128], P('dp', 'cp'), parts along dimension 0
Outputs:
- output 1: bfloat16 [4, 8192, 40, 128], P('dp', 'cp'), parts along dimension 0
- output 2: bfloat16 [4, 8192, 40, 128], P('dp', 'cp'), parts along dimension 0
- output 3: bfloat16 [4, 8192, 8, 128], P('dp', 'cp'), parts along dimension 0
- output 4: bfloat16 [4, 8192, 8, 128], P('dp', 'cp'), parts along dimension 0
There are 4 independent parts. The reference program is written for one: setup_inputs(seed, part) draws one part's arguments, and reference() takes and returns one part's arrays. A program takes and returns all parts, laid end to end along the dimension named above; each array names one.
All inputs are finite; a program needn't handle non-finite values.
Results may differ from the reference program's by a relative error of at most 0.00808623.
Values are sent between devices in bfloat16 or wider.
A program may use at most 768 MiB of HBM per device.

```python
import jax
import jax.numpy as jnp
from jax import lax

BATCH = 1
SEQ = 8192
HEADS = 40
KV_HEADS = 8
HEAD = 128
BLOCK = 64
LOCAL = 16
STRIDE = 8

GROUP = HEADS // KV_HEADS
HALO = (LOCAL - 1) * BLOCK
WINDOW = LOCAL * BLOCK
SCALE = 1.0 / HEAD


def setup_inputs(seed: int = 0, part: int = 0) -> dict:
    rng_key = jax.random.fold_in(jax.random.key(seed), part)
    key_q, key_k, key_v, key_d = jax.random.split(rng_key, 4)
    qk_std = 1.6 * HEAD ** 0.25
    q_shape = (BATCH, SEQ, HEADS, HEAD)
    kv_shape = (BATCH, SEQ, KV_HEADS, HEAD)
    q_rope = (qk_std * jax.random.normal(key_q, q_shape, jnp.float32)).astype(jnp.bfloat16)
    k_rope = (qk_std * jax.random.normal(key_k, kv_shape, jnp.float32)).astype(jnp.bfloat16)
    values = jax.random.normal(key_v, kv_shape, jnp.float32).astype(jnp.bfloat16)
    d_out = jax.random.normal(key_d, q_shape, jnp.float32).astype(jnp.bfloat16)
    return {'q_rope': q_rope, 'k_rope': k_rope, 'values': values, 'd_out': d_out}


def residue_table():
    head_ids = jnp.arange(KV_HEADS)[:, None] * GROUP + jnp.arange(GROUP)[None, :]
    return (-1 - head_ids) % STRIDE


def select_matrix():
    return (jnp.arange(STRIDE)[None, None, :] == residue_table()[:, :, None]).astype(jnp.float32)


def compact(keys_in):
    grouped = keys_in.astype(jnp.float32).reshape(BATCH, SEQ // (BLOCK * STRIDE), STRIDE, BLOCK, KV_HEADS, HEAD)
    picked = jnp.einsum('bmsigd,gus->bmigud', grouped, select_matrix())
    return picked.reshape(BATCH, SEQ // STRIDE, KV_HEADS, GROUP, HEAD)


def expand(grads):
    grouped = grads.reshape(BATCH, SEQ // (BLOCK * STRIDE), BLOCK, KV_HEADS, GROUP, HEAD)
    spread = jnp.einsum('bmigud,gus->bmsigd', grouped, select_matrix())
    return spread.reshape(BATCH, SEQ, KV_HEADS, HEAD)


def block_pass(q_rope, d_out, k_ext, v_ext, k_str, v_str):
    str_block = (jnp.arange(SEQ // STRIDE) // BLOCK)[None, None, :] * STRIDE + residue_table()[:, :, None]
    row_ids = jnp.arange(BLOCK)[:, None]
    col_ids = jnp.arange(WINDOW)[None, :]
    blk_shape = (BATCH, BLOCK, KV_HEADS, GROUP, HEAD)

    def body(carry, blk_idx):
        dk_ext, dv_ext, dk_str, dv_str = carry
        win_start = blk_idx * BLOCK
        q_blk = lax.dynamic_slice_in_dim(q_rope, win_start, BLOCK, axis=1).astype(jnp.float32).reshape(blk_shape)
        do_blk = lax.dynamic_slice_in_dim(d_out, win_start, BLOCK, axis=1).astype(jnp.float32).reshape(blk_shape)
        k_win = lax.dynamic_slice_in_dim(k_ext, win_start, WINDOW, axis=1)
        v_win = lax.dynamic_slice_in_dim(v_ext, win_start, WINDOW, axis=1)
        loc_mask = (col_ids <= row_ids + HALO) & (col_ids >= HALO - blk_idx * BLOCK)
        str_mask = (str_block <= blk_idx - LOCAL)[:, :, None, :]
        s_loc = jnp.where(loc_mask, jnp.einsum('bigud,bjgd->bguij', q_blk, k_win) * SCALE, -jnp.inf)
        s_str = jnp.where(str_mask, jnp.einsum('bigud,bjgud->bguij', q_blk, k_str) * SCALE, -jnp.inf)
        row_max = jnp.maximum(jnp.max(s_loc, axis=-1), jnp.max(s_str, axis=-1))[..., None]
        e_loc = jnp.exp(s_loc - row_max)
        e_str = jnp.exp(s_str - row_max)
        row_sum = jnp.sum(e_loc, axis=-1, keepdims=True) + jnp.sum(e_str, axis=-1, keepdims=True)
        p_loc = e_loc / row_sum
        p_str = e_str / row_sum
        pb_loc = p_loc.astype(jnp.bfloat16).astype(jnp.float32)
        pb_str = p_str.astype(jnp.bfloat16).astype(jnp.float32)
        o_blk = jnp.einsum('bguij,bjgd->bigud', pb_loc, v_win) + jnp.einsum('bguij,bjgud->bigud', pb_str, v_str)
        row_delta = jnp.einsum('bigud,bigud->bgui', do_blk, o_blk)[..., None]
        dp_loc = jnp.einsum('bigud,bjgd->bguij', do_blk, v_win)
        dp_str = jnp.einsum('bigud,bjgud->bguij', do_blk, v_str)
        ds_loc = (p_loc * (dp_loc - row_delta)).astype(jnp.bfloat16).astype(jnp.float32)
        ds_str = (p_str * (dp_str - row_delta)).astype(jnp.bfloat16).astype(jnp.float32)
        dq_blk = (jnp.einsum('bguij,bjgd->bigud', ds_loc, k_win) + jnp.einsum('bguij,bjgud->bigud', ds_str, k_str)) * SCALE
        dk_win = jnp.einsum('bguij,bigud->bjgd', ds_loc, q_blk) * SCALE
        dv_win = jnp.einsum('bguij,bigud->bjgd', pb_loc, do_blk)
        dk_ext = lax.dynamic_update_slice_in_dim(dk_ext, lax.dynamic_slice_in_dim(dk_ext, win_start, WINDOW, axis=1) + dk_win, win_start, axis=1)
        dv_ext = lax.dynamic_update_slice_in_dim(dv_ext, lax.dynamic_slice_in_dim(dv_ext, win_start, WINDOW, axis=1) + dv_win, win_start, axis=1)
        dk_str = dk_str + jnp.einsum('bguij,bigud->bjgud', ds_str, q_blk) * SCALE
        dv_str = dv_str + jnp.einsum('bguij,bigud->bjgud', pb_str, do_blk)
        return (dk_ext, dv_ext, dk_str, dv_str), (o_blk.astype(jnp.bfloat16), dq_blk.astype(jnp.bfloat16))

    init = (jnp.zeros(k_ext.shape, jnp.float32), jnp.zeros(v_ext.shape, jnp.float32), jnp.zeros(k_str.shape, jnp.float32), jnp.zeros(v_str.shape, jnp.float32))
    carry, stacked = lax.scan(body, init, jnp.arange(SEQ // BLOCK))
    attn_out = jnp.moveaxis(stacked[0], 0, 1).reshape(BATCH, SEQ, HEADS, HEAD)
    d_q = jnp.moveaxis(stacked[1], 0, 1).reshape(BATCH, SEQ, HEADS, HEAD)
    return (attn_out, d_q) + carry


def reference(q_rope, k_rope, values, d_out):
    pad_widths = ((0, 0), (HALO, 0), (0, 0), (0, 0))
    k_ext = jnp.pad(k_rope, pad_widths).astype(jnp.float32)
    v_ext = jnp.pad(values, pad_widths).astype(jnp.float32)
    attn_out, d_q, dk_ext, dv_ext, dk_str, dv_str = block_pass(q_rope, d_out, k_ext, v_ext, compact(k_rope), compact(values))
    d_k = dk_ext[:, HALO:] + expand(dk_str)
    d_v = dv_ext[:, HALO:] + expand(dv_str)
    return (attn_out, d_q, d_k.astype(jnp.bfloat16), d_v.astype(jnp.bfloat16))
```

```python
import functools

import jax
import jax.numpy as jnp
from jax import lax
from jax.experimental import pallas as pl
from jax.experimental.pallas import tpu as pltpu
from jax.sharding import PartitionSpec as P

BLOCK = 64
LOCAL = 16
STRIDE = 8
HALO = (LOCAL - 1) * BLOCK
ROWS = 256
CHUNK = 128
LOG2E = 1.4426950408889634
CHUNKS = 2
F32 = jnp.float32
BF16 = jnp.bfloat16


def residue(kv_head, member, group_size):
    return (-1 - (kv_head * group_size + member)) % STRIDE


def fold(x, op):
    rows, cols = x.shape
    return op(x.reshape(rows // 8, 8, cols), axis=0)


def pieces(total):
    return [(start, min(CHUNK, total - start)) for start in range(0, total, CHUNK)]


def attention_kernel(first_head, group_size, q_ref, do_ref, k_ref, v_ref, ks_ref, vs_ref,
                     o_ref, dq_ref, dk_own_ref, dv_own_ref, dk_halo_ref, dv_halo_ref, dks_ref, dvs_ref,
                     k_t, v_t, ks_t, vs_t, dk_acc, dv_acc, e_loc, e_str, pb_loc, pb_str, ds_loc, ds_str):
    shard = lax.axis_index('cp')
    head_idx, member = pl.program_id(0), pl.program_id(1)
    seq_loc, head_dim = q_ref.shape[2], q_ref.shape[3]
    n_tiles = seq_loc // ROWS
    win = HALO + ROWS
    win_pad = pb_loc.shape[1]
    n_str = ks_t.shape[1]
    scale = 1.0 / head_dim
    to_exp2 = scale * LOG2E
    jres = lax.rem(STRIDE * 64 - 1 - ((first_head + head_idx) * group_size + member), STRIDE)
    neg = -jnp.inf

    @pl.when((head_idx == 0) & (member == 0))
    def _():
        for t in range(n_tiles):
            pb_loc[t, win:, :] = jnp.zeros((win_pad - win, ROWS), BF16)
            ds_loc[t, win:, :] = jnp.zeros((win_pad - win, ROWS), BF16)

    @pl.when(member == 0)
    def _():
        k_t[...] = k_ref[0, 0].T
        v_t[...] = v_ref[0, 0].T
        dk_acc[...] = jnp.zeros_like(dk_acc)
        dv_acc[...] = jnp.zeros_like(dv_acc)

    def str_rows(ref, start, size):
        return ref[start // BLOCK:(start + size) // BLOCK, 0, 0, 0].reshape(size, head_dim)

    ks_t[...] = str_rows(ks_ref, 0, n_str).T
    vs_t[...] = str_rows(vs_ref, 0, n_str).T

    y_row = lax.broadcasted_iota(jnp.int32, (1, ROWS), 1)
    st = [dict() for _ in range(n_tiles)]
    for t in range(n_tiles):
        st[t]['q_t'] = q_ref[0, 0, t * ROWS:(t + 1) * ROWS, :].T
        st[t]['do_t'] = do_ref[0, 0, t * ROWS:(t + 1) * ROWS, :].T
        st[t]['thr'] = shard - 1 - ((y_row // BLOCK + t * (ROWS // BLOCK)) < jres).astype(jnp.int32)

    def score_steps(t):
        s = st[t]

        def local(start, size):
            def run():
                sc = jnp.dot(k_ref[0, 0, t * ROWS + start:t * ROWS + start + size, :], s['q_t'], preferred_element_type=F32)
                for off in range(0, size, BLOCK):
                    x0 = start + off
                    sub = sc[off:off + BLOCK]
                    if x0 < HALO:
                        seen = t * ROWS + x0 >= HALO - seq_loc * shard
                        sub = sub + jnp.where(seen, 0.0, neg).astype(F32)
                    if x0 < ROWS - BLOCK:
                        sub = jnp.where(y_row < x0 + BLOCK, sub, neg)
                    if x0 >= HALO:
                        col = lax.broadcasted_iota(jnp.int32, (BLOCK, ROWS), 0)
                        row = lax.broadcasted_iota(jnp.int32, (BLOCK, ROWS), 1)
                        sub = jnp.where(col + (x0 - HALO) <= row, sub, neg)
                    e_loc[t, x0:x0 + BLOCK, :] = sub
                    part = fold(sub, jnp.max)
                    s['mx'] = part if 'mx' not in s else jnp.maximum(s['mx'], part)
            return run

        def strided(start, size):
            def run():
                sc = jnp.dot(str_rows(ks_ref, start, size), s['q_t'], preferred_element_type=F32)
                for off in range(0, size, BLOCK):
                    x0 = start + off
                    sub = sc[off:off + BLOCK] + jnp.where(x0 // BLOCK < s['thr'], 0.0, neg).astype(F32)
                    e_str[t, x0:x0 + BLOCK, :] = sub
                    s['mx'] = jnp.maximum(s['mx'], fold(sub, jnp.max))
            return run

        def finish():
            s['m'] = jnp.max(s['mx'], axis=0, keepdims=True)
        return [local(*p) for p in pieces(win)] + [strided(*p) for p in pieces(n_str)] + [finish]

    def exp_steps(t):
        s = st[t]

        def one(ref, start, size):
            def run():
                e = jnp.exp2((ref[t, start:start + size, :] - s['m']) * to_exp2)
                ref[t, start:start + size, :] = e
                part = fold(e, jnp.sum)
                s['l'] = part if 'l' not in s else s['l'] + part
            return run

        def finish():
            s['inv'] = 1.0 / jnp.sum(s['l'], axis=0, keepdims=True)
        return [one(e_loc, *p) for p in pieces(win)] + [one(e_str, *p) for p in pieces(n_str)] + [finish]

    def out_steps(t):
        s = st[t]

        def loc(start, size):
            def run():
                pb_loc[t, start:start + size, :] = (e_loc[t, start:start + size, :] * s['inv']).astype(BF16)
            return run

        def strided(start, size):
            def run():
                pb_str[start:start + size, t * ROWS:(t + 1) * ROWS] = (e_str[t, start:start + size, :] * s['inv']).astype(BF16)
            return run

        def finish():
            o_t = (jnp.dot(v_t[:, t * ROWS:t * ROWS + win_pad], pb_loc[t], preferred_element_type=F32)
                   + jnp.dot(vs_t[...], pb_str[:, t * ROWS:(t + 1) * ROWS], preferred_element_type=F32))
            s['delta'] = jnp.sum(s['do_t'].astype(F32) * o_t, axis=0, keepdims=True)
            o_ref[0, 0, t * ROWS:(t + 1) * ROWS, :] = o_t.T.astype(BF16)
        return [loc(*p) for p in pieces(win)] + [strided(*p) for p in pieces(n_str)] + [finish]

    def grad_steps(t):
        s = st[t]

        def loc(start, size):
            def run():
                dp = jnp.dot(v_ref[0, 0, t * ROWS + start:t * ROWS + start + size, :], s['do_t'], preferred_element_type=F32)
                p = e_loc[t, start:start + size, :] * s['inv']
                ds_loc[t, start:start + size, :] = (p * (dp - s['delta'])).astype(BF16)
            return run

        def strided(start, size):
            def run():
                dp = jnp.dot(str_rows(vs_ref, start, size), s['do_t'], preferred_element_type=F32)
                p = e_str[t, start:start + size, :] * s['inv']
                ds_str[start:start + size, t * ROWS:(t + 1) * ROWS] = (p * (dp - s['delta'])).astype(BF16)
            return run
        return [loc(*p) for p in pieces(win)] + [strided(*p) for p in pieces(n_str)]

    def back_steps(t):
        def dv():
            dv_acc[t * ROWS:t * ROWS + win, :] += jnp.dot(pb_loc[t, :win, :], do_ref[0, 0, t * ROWS:(t + 1) * ROWS, :], preferred_element_type=F32)

        def dk():
            dk_acc[t * ROWS:t * ROWS + win, :] += jnp.dot(ds_loc[t, :win, :], q_ref[0, 0, t * ROWS:(t + 1) * ROWS, :], preferred_element_type=F32)

        def dq():
            dq_t = (jnp.dot(k_t[:, t * ROWS:t * ROWS + win_pad], ds_loc[t], preferred_element_type=F32)
                    + jnp.dot(ks_t[...], ds_str[:, t * ROWS:(t + 1) * ROWS], preferred_element_type=F32))
            dq_ref[0, 0, t * ROWS:(t + 1) * ROWS, :] = (dq_t * scale).T.astype(BF16)
        return [dv, dk, dq]

    def weave(*lists):
        total = max(len(x) for x in lists)
        for i in range(total):
            for x in lists:
                for j in range(i * len(x) // total, (i + 1) * len(x) // total):
                    x[j]()

    weave(score_steps(0))
    for t in range(n_tiles):
        later = score_steps(t + 1) if t + 1 < n_tiles else []
        earlier = back_steps(t - 1) if t > 0 else []
        weave(*[x for x in (exp_steps(t), later, earlier) if x])
        weave(out_steps(t))
        weave(grad_steps(t))
    weave(back_steps(n_tiles - 1))

    n_blk = n_str // BLOCK
    dvs = jnp.dot(pb_str[...], do_ref[0, 0], preferred_element_type=F32)
    dvs_ref[:n_blk, 0, 0] = dvs.reshape(n_blk, BLOCK, head_dim)
    dks = jnp.dot(ds_str[...], q_ref[0, 0], preferred_element_type=F32) * scale
    dks_ref[:n_blk, 0, 0] = dks.reshape(n_blk, BLOCK, head_dim)
    rest = dks_ref.shape[0] - n_blk
    dks_ref[n_blk:, 0, 0] = jnp.zeros((rest, BLOCK, head_dim), F32)
    dvs_ref[n_blk:, 0, 0] = jnp.zeros((rest, BLOCK, head_dim), F32)

    @pl.when(member == group_size - 1)
    def _():
        dk_own_ref[0] = dk_acc[HALO:HALO + seq_loc, :] * scale
        dv_own_ref[0] = dv_acc[HALO:HALO + seq_loc, :]
        dk_halo_ref[0] = (dk_acc[:HALO, :] * scale).astype(BF16)
        dv_halo_ref[0] = dv_acc[:HALO, :].astype(BF16)


def attention(first_head, n_heads, q, d_out, kv_ext, kv_str):
    _, group_size, seq_loc, head_dim = q.shape
    ext_pad = kv_ext.shape[2]
    cp_size = kv_str.shape[0]
    n_blk = cp_size - 2
    n_str = n_blk * BLOCK
    win = HALO + ROWS
    win_pad = -(-win // 256) * 256
    n_tiles = seq_loc // ROWS
    spec_q = pl.BlockSpec((1, 1, seq_loc, head_dim), lambda g, u: (first_head + g, u, 0, 0))
    spec_o = pl.BlockSpec((1, 1, seq_loc, head_dim), lambda g, u: (g, u, 0, 0))
    ext = [pl.BlockSpec((1, 1, ext_pad, head_dim), lambda g, u, w=w: (w, first_head + g, 0, 0)) for w in range(2)]
    strided = [pl.BlockSpec((n_blk, 1, 1, 1, BLOCK, head_dim), lambda g, u, w=w: (0, w, g, u, 0, 0)) for w in range(2)]
    spec_own = pl.BlockSpec((1, seq_loc, head_dim), lambda g, u: (g, 0, 0))
    spec_halo = pl.BlockSpec((1, HALO, head_dim), lambda g, u: (g, 0, 0))
    spec_str = pl.BlockSpec((cp_size, 1, 1, BLOCK, head_dim), lambda g, u: (0, g, u, 0, 0))
    sds = jax.ShapeDtypeStruct
    flops = n_heads * group_size * 6 * 2 * seq_loc * (win + n_str) * head_dim
    return pl.pallas_call(
        functools.partial(attention_kernel, first_head, group_size),
        grid=(n_heads, group_size),
        in_specs=[spec_q, spec_q, ext[0], ext[1], strided[0], strided[1]],
        out_specs=[spec_o, spec_o, spec_own, spec_own, spec_halo, spec_halo, spec_str, spec_str],
        out_shape=[
            sds((n_heads, group_size, seq_loc, head_dim), BF16), sds((n_heads, group_size, seq_loc, head_dim), BF16),
            sds((n_heads, seq_loc, head_dim), F32), sds((n_heads, seq_loc, head_dim), F32),
            sds((n_heads, HALO, head_dim), BF16), sds((n_heads, HALO, head_dim), BF16),
            sds((cp_size, n_heads, group_size, BLOCK, head_dim), F32), sds((cp_size, n_heads, group_size, BLOCK, head_dim), F32),
        ],
        scratch_shapes=[
            pltpu.VMEM((head_dim, ext_pad), BF16), pltpu.VMEM((head_dim, ext_pad), BF16),
            pltpu.VMEM((head_dim, n_str), BF16), pltpu.VMEM((head_dim, n_str), BF16),
            pltpu.VMEM((HALO + seq_loc, head_dim), F32), pltpu.VMEM((HALO + seq_loc, head_dim), F32),
            pltpu.VMEM((n_tiles, win, ROWS), F32), pltpu.VMEM((n_tiles, n_str, ROWS), F32),
            pltpu.VMEM((n_tiles, win_pad, ROWS), BF16), pltpu.VMEM((n_str, seq_loc), BF16),
            pltpu.VMEM((n_tiles, win_pad, ROWS), BF16), pltpu.VMEM((n_str, seq_loc), BF16),
        ],
        compiler_params=pltpu.CompilerParams(vmem_limit_bytes=48 * 1024 * 1024),
        cost_estimate=pl.CostEstimate(flops=flops, bytes_accessed=0, transcendentals=0),
        name='attention',
    )(q, d_out, kv_ext, kv_ext, kv_str, kv_str)


def halo_lengths(seq_loc):
    hop_count = -(-HALO // seq_loc)
    return [seq_loc] * (hop_count - 1) + [HALO - (hop_count - 1) * seq_loc]


def solution(mesh):
    cp_size = mesh.shape['cp']
    spec = P('dp', 'cp', None, None)

    def per_device(q_rope, k_rope, values, d_out):
        seq_loc, heads, head_dim = q_rope.shape[1:]
        kv_heads = k_rope.shape[2]
        group_size = heads // kv_heads
        lengths = halo_lengths(seq_loc)
        n_res = seq_loc // BLOCK
        kv = jnp.stack([jnp.swapaxes(k_rope[0], 0, 1), jnp.swapaxes(values[0], 0, 1)])
        kvb = kv.reshape(2, kv_heads, n_res, BLOCK, head_dim)
        kv_c = jnp.stack([jnp.stack([kvb[:, g, residue(g, u, group_size)] for u in range(group_size)], 1) for g in range(kv_heads)], 1)
        parts = []
        for dist in range(len(lengths), 0, -1):
            tail = kv[:, :, seq_loc - lengths[dist - 1]:]
            parts.append(lax.ppermute(tail, 'cp', [(s, s + dist) for s in range(cp_size - dist)]))
        per = kv_heads // CHUNKS
        gathered = [lax.all_gather(kv_c[:, i * per:(i + 1) * per], 'cp', axis=0, tiled=False) for i in range(CHUNKS)]
        pad = -(HALO + seq_loc) % 256
        kv_ext = jnp.concatenate(parts + [kv, jnp.zeros((2, kv_heads, pad, head_dim), BF16)], axis=2)

        def head_major(x):
            return jnp.transpose(x[0].reshape(seq_loc, kv_heads, group_size, head_dim), (1, 2, 0, 3))

        q_h, do_h = head_major(q_rope), head_major(d_out)
        outs = [attention(i * per, per, q_h, do_h, kv_ext, gathered[i]) for i in range(CHUNKS)]
        strided = [[lax.psum_scatter(out[6 + w], 'cp', scatter_dimension=0, tiled=False) for out in outs] for w in range(2)]

        def token_major(xs):
            x = jnp.concatenate(xs, axis=0)
            return jnp.transpose(x, (2, 0, 1, 3)).reshape(1, seq_loc, heads, head_dim)

        attn_out = token_major([out[0] for out in outs])
        d_q = token_major([out[1] for out in outs])

        def finish(w):
            own = jnp.concatenate([out[2 + w] for out in outs], axis=0)
            halo = jnp.concatenate([out[4 + w] for out in outs], axis=0)
            offset = 0
            total = own
            for dist in range(len(lengths), 0, -1):
                size = lengths[dist - 1]
                arrived = lax.ppermute(halo[:, offset:offset + size], 'cp', [(s + dist, s) for s in range(cp_size - dist)])
                offset += size
                total = total + jnp.pad(arrived, ((0, 0), (seq_loc - size, 0), (0, 0))).astype(F32)
            got = jnp.concatenate(strided[w], axis=0)
            zero = jnp.zeros((BLOCK, head_dim), F32)
            rows = []
            for g in range(kv_heads):
                by_res = {residue(g, u, group_size): u for u in range(group_size)}
                rows.append(jnp.concatenate([got[g, by_res[r]] if r in by_res else zero for r in range(n_res)], axis=0))
            total = total + jnp.stack(rows)
            return jnp.swapaxes(total.astype(BF16), 0, 1)[None]

        return attn_out, d_q, finish(0), finish(1)

    return jax.shard_map(per_device, mesh=mesh, in_specs=(spec, spec, spec, spec), out_specs=(spec, spec, spec, spec), check_vma=False)
```

```python
import functools

import jax
import jax.numpy as jnp
from jax import lax
from jax.experimental import pallas as pl
from jax.experimental.pallas import tpu as pltpu
from jax.sharding import PartitionSpec as P

BLOCK = 64
LOCAL = 16
STRIDE = 8
HALO = (LOCAL - 1) * BLOCK
ROWS = 256
CHUNK = 128
LOG2E = 1.4426950408889634
CHUNKS = (2, 3, 3)
F32 = jnp.float32
BF16 = jnp.bfloat16


def fold(x, op):
    rows, cols = x.shape
    return op(x.reshape(rows // 8, 8, cols), axis=0)


def pieces(total):
    return [(start, min(CHUNK, total - start)) for start in range(0, total, CHUNK)]


def attention_kernel(info_ref, q_ref, do_ref, ko_ref, vo_ref, k1_ref, v1_ref, k2_ref, v2_ref, kr1_ref, vr1_ref, kr2_ref, vr2_ref, ks_ref, vs_ref,
                     o_ref, dq_ref, own_ref, rest1_ref, rest2_ref, str_ref,
                     k_ext, v_ext, k_t, v_t, ks_t, vs_t, dk_acc, dv_acc, e_loc, e_str, pb_loc, pb_str, ds_loc, ds_str):
    shard = info_ref[1]
    head_idx, member = pl.program_id(0), pl.program_id(1)
    group_size = str_ref.shape[3]
    seq_loc, head_dim = q_ref.shape[2], q_ref.shape[3]
    n_res = seq_loc // BLOCK
    n_tiles = seq_loc // ROWS
    win = HALO + ROWS
    win_pad = pb_loc.shape[1]
    n_str = ks_t.shape[1]
    n_blk = n_str // BLOCK
    scale = 1.0 / head_dim
    to_exp2 = scale * LOG2E
    neg = -jnp.inf

    def res_of(slot):
        return lax.rem(STRIDE * 64 - 1 - ((info_ref[0] + head_idx) * group_size + slot), STRIDE)

    def rows_at(block):
        return pl.ds(pl.multiple_of(block * BLOCK, BLOCK), BLOCK)

    jres = res_of(member)

    @pl.when((head_idx == 0) & (member == 0))
    def _():
        for t in range(n_tiles):
            pb_loc[t, win:, :] = jnp.zeros((win_pad - win, ROWS), BF16)
            ds_loc[t, win:, :] = jnp.zeros((win_pad - win, ROWS), BF16)

    @pl.when(member == 0)
    def _():
        for ext, own, near, far, near_rest, far_rest in ((k_ext, ko_ref, k1_ref, k2_ref, kr1_ref, kr2_ref), (v_ext, vo_ref, v1_ref, v2_ref, vr1_ref, vr2_ref)):
            for slot in range(n_res):
                res = res_of(slot)
                far_blk = far[0, 0, 0, slot] if slot < group_size else far_rest[0, 0, slot - group_size]
                near_blk = near[0, 0, 0, slot] if slot < group_size else near_rest[0, 0, slot - group_size]
                ext[rows_at(res), :] = far_blk
                ext[rows_at(res + n_res), :] = near_blk
                ext[rows_at(res + 2 * n_res), :] = own[0, 0, slot]
        k_t[...] = jnp.zeros_like(k_t)
        v_t[...] = jnp.zeros_like(v_t)
        k_t[:, :HALO + seq_loc] = k_ext[BLOCK:, :].T
        v_t[:, :HALO + seq_loc] = v_ext[BLOCK:, :].T
        dk_acc[...] = jnp.zeros_like(dk_acc)
        dv_acc[...] = jnp.zeros_like(dv_acc)
        str_ref[n_blk:] = jnp.zeros((str_ref.shape[0] - n_blk,) + str_ref.shape[1:], F32)

    def str_rows(ref, start, size):
        return ref[start // BLOCK:(start + size) // BLOCK, 0, 0, 0].reshape(size, head_dim)

    def ext_rows(ref, start, size):
        return ref[BLOCK + start:BLOCK + start + size, :]

    ks_t[...] = str_rows(ks_ref, 0, n_str).T
    vs_t[...] = str_rows(vs_ref, 0, n_str).T

    y_row = lax.broadcasted_iota(jnp.int32, (1, ROWS), 1)
    st = [dict() for _ in range(n_tiles)]
    for t in range(n_tiles):
        st[t]['q_t'] = q_ref[0, 0, t * ROWS:(t + 1) * ROWS, :].T
        st[t]['do_t'] = do_ref[0, 0, t * ROWS:(t + 1) * ROWS, :].T
        st[t]['thr'] = shard - 1 - ((y_row // BLOCK + t * (ROWS // BLOCK)) < jres).astype(jnp.int32)

    def score_steps(t):
        s = st[t]

        def local(start, size):
            def run():
                sc = jnp.dot(ext_rows(k_ext, t * ROWS + start, size), s['q_t'], preferred_element_type=F32)
                for off in range(0, size, BLOCK):
                    x0 = start + off
                    sub = sc[off:off + BLOCK]
                    if x0 < HALO:
                        seen = t * ROWS + x0 >= HALO - seq_loc * shard
                        sub = sub + jnp.where(seen, 0.0, neg).astype(F32)
                    if x0 < ROWS - BLOCK:
                        sub = jnp.where(y_row < x0 + BLOCK, sub, neg)
                    if x0 >= HALO:
                        col = lax.broadcasted_iota(jnp.int32, (BLOCK, ROWS), 0)
                        row = lax.broadcasted_iota(jnp.int32, (BLOCK, ROWS), 1)
                        sub = jnp.where(col + (x0 - HALO) <= row, sub, neg)
                    e_loc[t, x0:x0 + BLOCK, :] = sub
                    part = fold(sub, jnp.max)
                    s['mx'] = part if 'mx' not in s else jnp.maximum(s['mx'], part)
            return run

        def strided(start, size):
            def run():
                sc = jnp.dot(str_rows(ks_ref, start, size), s['q_t'], preferred_element_type=F32)
                for off in range(0, size, BLOCK):
                    x0 = start + off
                    sub = sc[off:off + BLOCK] + jnp.where(x0 // BLOCK < s['thr'], 0.0, neg).astype(F32)
                    e_str[t, x0:x0 + BLOCK, :] = sub
                    s['mx'] = jnp.maximum(s['mx'], fold(sub, jnp.max))
            return run

        def finish():
            s['m'] = jnp.max(s['mx'], axis=0, keepdims=True)
        return [local(*p) for p in pieces(win)] + [strided(*p) for p in pieces(n_str)] + [finish]

    def exp_steps(t):
        s = st[t]

        def one(ref, start, size):
            def run():
                e = jnp.exp2((ref[t, start:start + size, :] - s['m']) * to_exp2)
                ref[t, start:start + size, :] = e
                part = fold(e, jnp.sum)
                s['l'] = part if 'l' not in s else s['l'] + part
            return run

        def finish():
            s['inv'] = 1.0 / jnp.sum(s['l'], axis=0, keepdims=True)
        return [one(e_loc, *p) for p in pieces(win)] + [one(e_str, *p) for p in pieces(n_str)] + [finish]

    def out_steps(t):
        s = st[t]

        def loc(start, size):
            def run():
                pb_loc[t, start:start + size, :] = (e_loc[t, start:start + size, :] * s['inv']).astype(BF16)
            return run

        def strided(start, size):
            def run():
                pb_str[start:start + size, t * ROWS:(t + 1) * ROWS] = (e_str[t, start:start + size, :] * s['inv']).astype(BF16)
            return run

        def finish():
            o_t = (jnp.dot(v_t[:, t * ROWS:t * ROWS + win_pad], pb_loc[t], preferred_element_type=F32)
                   + jnp.dot(vs_t[...], pb_str[:, t * ROWS:(t + 1) * ROWS], preferred_element_type=F32))
            s['delta'] = jnp.sum(s['do_t'].astype(F32) * o_t, axis=0, keepdims=True)
            o_ref[0, 0, t * ROWS:(t + 1) * ROWS, :] = o_t.T.astype(BF16)
        return [loc(*p) for p in pieces(win)] + [strided(*p) for p in pieces(n_str)] + [finish]

    def grad_steps(t):
        s = st[t]

        def loc(start, size):
            def run():
                dp = jnp.dot(ext_rows(v_ext, t * ROWS + start, size), s['do_t'], preferred_element_type=F32)
                p = e_loc[t, start:start + size, :] * s['inv']
                ds_loc[t, start:start + size, :] = (p * (dp - s['delta'])).astype(BF16)
            return run

        def strided(start, size):
            def run():
                dp = jnp.dot(str_rows(vs_ref, start, size), s['do_t'], preferred_element_type=F32)
                p = e_str[t, start:start + size, :] * s['inv']
                ds_str[start:start + size, t * ROWS:(t + 1) * ROWS] = (p * (dp - s['delta'])).astype(BF16)
            return run
        return [loc(*p) for p in pieces(win)] + [strided(*p) for p in pieces(n_str)]

    def back_steps(t):
        def dv():
            dv_acc[BLOCK + t * ROWS:BLOCK + t * ROWS + win, :] += jnp.dot(pb_loc[t, :win, :], do_ref[0, 0, t * ROWS:(t + 1) * ROWS, :], preferred_element_type=F32)

        def dk():
            dk_acc[BLOCK + t * ROWS:BLOCK + t * ROWS + win, :] += jnp.dot(ds_loc[t, :win, :], q_ref[0, 0, t * ROWS:(t + 1) * ROWS, :], preferred_element_type=F32)

        def dq():
            dq_t = (jnp.dot(k_t[:, t * ROWS:t * ROWS + win_pad], ds_loc[t], preferred_element_type=F32)
                    + jnp.dot(ks_t[...], ds_str[:, t * ROWS:(t + 1) * ROWS], preferred_element_type=F32))
            dq_ref[0, 0, t * ROWS:(t + 1) * ROWS, :] = (dq_t * scale).T.astype(BF16)
        return [dv, dk, dq]

    def weave(*lists):
        total = max(len(x) for x in lists)
        for i in range(total):
            for x in lists:
                for j in range(i * len(x) // total, (i + 1) * len(x) // total):
                    x[j]()

    weave(score_steps(0))
    for t in range(n_tiles):
        later = score_steps(t + 1) if t + 1 < n_tiles else []
        earlier = back_steps(t - 1) if t > 0 else []
        weave(*[x for x in (exp_steps(t), later, earlier) if x])
        weave(out_steps(t))
        weave(grad_steps(t))
    weave(back_steps(n_tiles - 1))

    str_ref[:n_blk, 1, 0, member] = jnp.dot(pb_str[...], do_ref[0, 0], preferred_element_type=F32).reshape(n_blk, BLOCK, head_dim)
    dks = jnp.dot(ds_str[...], q_ref[0, 0], preferred_element_type=F32) * scale
    str_ref[:n_blk, 0, 0, member] = dks.reshape(n_blk, BLOCK, head_dim)

    @pl.when(member == group_size - 1)
    def _():
        near_dev = jnp.maximum(shard - 1, 0)
        far_dev = jnp.maximum(shard - 2, 0)
        for w, acc, factor in ((0, dk_acc, scale), (1, dv_acc, 1.0)):
            for slot in range(n_res):
                res = res_of(slot)
                far = acc[rows_at(res), :] * factor
                near = acc[rows_at(res + n_res), :] * factor
                own_ref[w, 0, slot] = acc[rows_at(res + 2 * n_res), :] * factor
                if slot < group_size:
                    str_ref[far_dev, w, 0, slot] += far
                    str_ref[near_dev, w, 0, slot] += near
                else:
                    rest2_ref[w, 0, slot - group_size] = far.astype(BF16)
                    rest1_ref[w, 0, slot - group_size] = near.astype(BF16)


def attention(first_head, n_heads, shard, q, d_out, kv_rot, rest1, rest2, gathered):
    _, group_size, seq_loc, head_dim = q.shape
    n_res = seq_loc // BLOCK
    n_rest = n_res - group_size
    cp_size = gathered.shape[0]
    n_blk = cp_size - 2
    n_str = n_blk * BLOCK
    win = HALO + ROWS
    win_pad = -(-win // 256) * 256
    n_tiles = seq_loc // ROWS
    ext_len = BLOCK + HALO + seq_loc
    ext_pad = (n_tiles - 1) * ROWS + win_pad
    spec_q = pl.BlockSpec((1, 1, seq_loc, head_dim), lambda g, u, s: (s[0] + g, u, 0, 0))
    spec_o = pl.BlockSpec((1, 1, seq_loc, head_dim), lambda g, u, s: (g, u, 0, 0))
    own = [pl.BlockSpec((1, 1, n_res, BLOCK, head_dim), lambda g, u, s, w=w: (w, s[0] + g, 0, 0, 0)) for w in range(2)]
    prev = [[pl.BlockSpec((1, 1, 1, group_size, BLOCK, head_dim), lambda g, u, s, w=w, d=d: (jnp.maximum(s[1] - d, 0), w, g, 0, 0, 0)) for w in range(2)] for d in (1, 2)]
    rest = [pl.BlockSpec((1, 1, n_rest, BLOCK, head_dim), lambda g, u, s, w=w: (w, s[0] + g, 0, 0, 0)) for w in range(2)]
    strided = [pl.BlockSpec((n_blk, 1, 1, 1, BLOCK, head_dim), lambda g, u, s, w=w: (0, w, g, u, 0, 0)) for w in range(2)]
    spec_own = pl.BlockSpec((2, 1, n_res, BLOCK, head_dim), lambda g, u, s: (0, g, 0, 0, 0))
    spec_rest = pl.BlockSpec((2, 1, n_rest, BLOCK, head_dim), lambda g, u, s: (0, g, 0, 0, 0))
    spec_str = pl.BlockSpec((cp_size, 2, 1, group_size, BLOCK, head_dim), lambda g, u, s: (0, 0, g, 0, 0, 0))
    sds = jax.ShapeDtypeStruct
    flops = n_heads * group_size * 6 * 2 * seq_loc * (win + n_str) * head_dim
    info = jnp.stack([jnp.int32(first_head), shard.astype(jnp.int32)])
    return pl.pallas_call(
        attention_kernel,
        grid_spec=pltpu.PrefetchScalarGridSpec(
            num_scalar_prefetch=1,
            grid=(n_heads, group_size),
            in_specs=[spec_q, spec_q, *own, *prev[0], *prev[1], *rest, *rest, *strided],
            out_specs=[spec_o, spec_o, spec_own, spec_rest, spec_rest, spec_str],
            scratch_shapes=[
                pltpu.VMEM((ext_len, head_dim), BF16), pltpu.VMEM((ext_len, head_dim), BF16),
                pltpu.VMEM((head_dim, ext_pad), BF16), pltpu.VMEM((head_dim, ext_pad), BF16),
                pltpu.VMEM((head_dim, n_str), BF16), pltpu.VMEM((head_dim, n_str), BF16),
                pltpu.VMEM((ext_len, head_dim), F32), pltpu.VMEM((ext_len, head_dim), F32),
                pltpu.VMEM((n_tiles, win, ROWS), F32), pltpu.VMEM((n_tiles, n_str, ROWS), F32),
                pltpu.VMEM((n_tiles, win_pad, ROWS), BF16), pltpu.VMEM((n_str, seq_loc), BF16),
                pltpu.VMEM((n_tiles, win_pad, ROWS), BF16), pltpu.VMEM((n_str, seq_loc), BF16),
            ]),
        out_shape=[
            sds((n_heads, group_size, seq_loc, head_dim), BF16), sds((n_heads, group_size, seq_loc, head_dim), BF16),
            sds((2, n_heads, n_res, BLOCK, head_dim), F32),
            sds((2, n_heads, n_rest, BLOCK, head_dim), BF16), sds((2, n_heads, n_rest, BLOCK, head_dim), BF16),
            sds((cp_size, 2, n_heads, group_size, BLOCK, head_dim), F32),
        ],
        compiler_params=pltpu.CompilerParams(vmem_limit_bytes=56 * 1024 * 1024),
        cost_estimate=pl.CostEstimate(flops=flops, bytes_accessed=0, transcendentals=0),
        name='attention',
    )(info, q, d_out, kv_rot, kv_rot, gathered, gathered, gathered, gathered, rest1, rest1, rest2, rest2, gathered, gathered)


def rotate_kernel(group_size, k_ref, v_ref, out_ref):
    n_res = out_ref.shape[2]
    for w, ref in enumerate((k_ref, v_ref)):
        for slot in range(n_res):
            res = lax.rem(STRIDE * 64 - 1 - (pl.program_id(0) * group_size + slot), STRIDE)
            out_ref[w, 0, slot] = ref[0, pl.ds(pl.multiple_of(res * BLOCK, BLOCK), BLOCK), :]


def rotate(k_h, v_h, group_size):
    kv_heads, seq_loc, head_dim = k_h.shape
    n_res = seq_loc // BLOCK
    spec = pl.BlockSpec((1, seq_loc, head_dim), lambda g: (g, 0, 0))
    return pl.pallas_call(
        functools.partial(rotate_kernel, group_size),
        grid=(kv_heads,),
        in_specs=[spec, spec],
        out_specs=pl.BlockSpec((2, 1, n_res, BLOCK, head_dim), lambda g: (0, g, 0, 0, 0)),
        out_shape=jax.ShapeDtypeStruct((2, kv_heads, n_res, BLOCK, head_dim), BF16),
        cost_estimate=pl.CostEstimate(flops=10 ** 7, bytes_accessed=0, transcendentals=0),
        name='rotate',
    )(k_h, v_h)


def merge_kernel(first_head, own_ref, red_ref, back1_ref, back2_ref, out_ref):
    n_res, group_size = own_ref.shape[2], red_ref.shape[2]
    for w in range(2):
        for slot in range(n_res):
            res = lax.rem(STRIDE * 64 - 1 - ((first_head + pl.program_id(0)) * group_size + slot), STRIDE)
            if slot < group_size:
                total = own_ref[w, 0, slot] + red_ref[w, 0, slot]
            else:
                total = own_ref[w, 0, slot] + back1_ref[w, 0, slot - group_size].astype(F32) + back2_ref[w, 0, slot - group_size].astype(F32)
            out_ref[w, 0, pl.ds(pl.multiple_of(res * BLOCK, BLOCK), BLOCK), :] = total.astype(BF16)


def merge(first_head, own, reduced, back1, back2):
    _, n_heads, n_res, _, head_dim = own.shape
    group_size, n_rest = reduced.shape[2], back1.shape[2]
    seq_loc = n_res * BLOCK

    def spec(count):
        return pl.BlockSpec((2, 1, count, BLOCK, head_dim), lambda g: (0, g, 0, 0, 0))
    return pl.pallas_call(
        functools.partial(merge_kernel, first_head),
        grid=(n_heads,),
        in_specs=[spec(n_res), spec(group_size), spec(n_rest), spec(n_rest)],
        out_specs=pl.BlockSpec((2, 1, seq_loc, head_dim), lambda g: (0, g, 0, 0)),
        out_shape=jax.ShapeDtypeStruct((2, n_heads, seq_loc, head_dim), BF16),
        cost_estimate=pl.CostEstimate(flops=10 ** 7, bytes_accessed=0, transcendentals=0),
        name='merge',
    )(own, reduced, back1, back2)


def solution(mesh):
    cp_size = mesh.shape['cp']
    spec = P('dp', 'cp', None, None)

    def per_device(q_rope, k_rope, values, d_out):
        seq_loc, heads, head_dim = q_rope.shape[1:]
        kv_heads = k_rope.shape[2]
        group_size = heads // kv_heads
        shard = lax.axis_index('cp')
        kv_rot = rotate(jnp.swapaxes(k_rope[0], 0, 1), jnp.swapaxes(values[0], 0, 1), group_size)
        starts = [sum(CHUNKS[:i]) for i in range(len(CHUNKS))]
        gathered = [lax.all_gather(kv_rot[:, a:a + n, :group_size], 'cp', axis=0, tiled=False) for a, n in zip(starts, CHUNKS)]
        rest = kv_rot[:, :, group_size:]
        rest1, rest2 = [lax.ppermute(rest, 'cp', [(s, s + dist) for s in range(cp_size - dist)]) for dist in (1, 2)]

        def head_major(x):
            return jnp.transpose(x[0].reshape(seq_loc, kv_heads, group_size, head_dim), (1, 2, 0, 3))

        q_h, do_h = head_major(q_rope), head_major(d_out)
        outs = [attention(a, n, shard, q_h, do_h, kv_rot, rest1, rest2, gathered[i]) for i, (a, n) in enumerate(zip(starts, CHUNKS))]
        reduced = [lax.psum_scatter(out[5], 'cp', scatter_dimension=0, tiled=False) for out in outs]

        def token_major(xs):
            x = jnp.concatenate(xs, axis=0)
            return jnp.transpose(x, (2, 0, 1, 3)).reshape(1, seq_loc, heads, head_dim)

        attn_out = token_major([out[0] for out in outs])
        d_q = token_major([out[1] for out in outs])

        merged = []
        for i, (out, red) in enumerate(zip(outs, reduced)):
            back = [lax.ppermute(out[2 + dist], 'cp', [(s + dist, s) for s in range(cp_size - dist)]) for dist in (1, 2)]
            merged.append(merge(starts[i], out[2], red, back[0], back[1]))
        plain = jnp.swapaxes(jnp.concatenate(merged, axis=1), 1, 2)
        return attn_out, d_q, plain[0][None], plain[1][None]

    return jax.shard_map(per_device, mesh=mesh, in_specs=(spec, spec, spec, spec), out_specs=(spec, spec, spec, spec), check_vma=False)
```

```python
import functools

import jax
import jax.numpy as jnp
from jax import lax
from jax.experimental import pallas as pl
from jax.experimental.pallas import tpu as pltpu
from jax.sharding import PartitionSpec as P

BLOCK = 64
LOCAL = 16
STRIDE = 8
HALO = (LOCAL - 1) * BLOCK
ROWS = 256
CHUNK = 128
LOG2E = 1.4426950408889634
CHUNKS = (2, 3, 3)
F32 = jnp.float32
BF16 = jnp.bfloat16


def fold(x, op):
    rows, cols = x.shape
    return op(x.reshape(rows // 8, 8, cols), axis=0)


def pieces(total):
    return [(start, min(CHUNK, total - start)) for start in range(0, total, CHUNK)]


def attention_kernel(info_ref, q_ref, do_ref, ko_ref, vo_ref, k1_ref, v1_ref, k2_ref, v2_ref, kr1_ref, vr1_ref, kr2_ref, vr2_ref, ks_ref, vs_ref,
                     o_ref, dq_ref, own_ref, rest1_ref, rest2_ref, str_ref,
                     k_ext, v_ext, k_t, v_t, ks_t, vs_t, dk_acc, dv_acc, e_loc, e_str, pb_loc, pb_str, ds_loc, ds_str):
    shard = info_ref[1]
    head_idx, member = pl.program_id(0), pl.program_id(1)
    group_size = str_ref.shape[3]
    seq_loc, head_dim = q_ref.shape[2], q_ref.shape[3]
    n_res = seq_loc // BLOCK
    n_tiles = seq_loc // ROWS
    win = HALO + ROWS
    win_pad = pb_loc.shape[1]
    n_str = ks_t.shape[1]
    n_blk = n_str // BLOCK
    scale = 1.0 / head_dim
    to_exp2 = scale * LOG2E
    neg = -jnp.inf

    def res_of(slot):
        return lax.rem(STRIDE * 64 - 1 - ((info_ref[0] + head_idx) * group_size + slot), STRIDE)

    def rows_at(block):
        return pl.ds(pl.multiple_of(block * BLOCK, BLOCK), BLOCK)

    jres = res_of(member)

    @pl.when((head_idx == 0) & (member == 0))
    def _():
        for t in range(n_tiles):
            pb_loc[t, win:, :] = jnp.zeros((win_pad - win, ROWS), BF16)
            ds_loc[t, win:, :] = jnp.zeros((win_pad - win, ROWS), BF16)

    @pl.when(member == 0)
    def _():
        for ext, own, near, far, near_rest, far_rest in ((k_ext, ko_ref, k1_ref, k2_ref, kr1_ref, kr2_ref), (v_ext, vo_ref, v1_ref, v2_ref, vr1_ref, vr2_ref)):
            for slot in range(n_res):
                res = res_of(slot)
                far_blk = far[0, 0, 0, slot] if slot < group_size else far_rest[0, 0, slot - group_size]
                near_blk = near[0, 0, 0, slot] if slot < group_size else near_rest[0, 0, slot - group_size]
                ext[rows_at(res), :] = far_blk
                ext[rows_at(res + n_res), :] = near_blk
                ext[rows_at(res + 2 * n_res), :] = own[0, 0, slot]
        k_t[...] = jnp.zeros_like(k_t)
        v_t[...] = jnp.zeros_like(v_t)
        k_t[:, :HALO + seq_loc] = k_ext[BLOCK:, :].T
        v_t[:, :HALO + seq_loc] = v_ext[BLOCK:, :].T
        dk_acc[...] = jnp.zeros_like(dk_acc)
        dv_acc[...] = jnp.zeros_like(dv_acc)
        str_ref[n_blk:] = jnp.zeros((str_ref.shape[0] - n_blk,) + str_ref.shape[1:], F32)

    def str_rows(ref, start, size):
        return ref[start // BLOCK:(start + size) // BLOCK, 0, 0, 0].reshape(size, head_dim)

    def ext_rows(ref, start, size):
        return ref[BLOCK + start:BLOCK + start + size, :]

    ks_t[...] = str_rows(ks_ref, 0, n_str).T
    vs_t[...] = str_rows(vs_ref, 0, n_str).T

    y_row = lax.broadcasted_iota(jnp.int32, (1, ROWS), 1)
    st = [dict() for _ in range(n_tiles)]
    for t in range(n_tiles):
        st[t]['q_t'] = q_ref[0, 0, t * ROWS:(t + 1) * ROWS, :].T
        st[t]['do_t'] = do_ref[0, 0, t * ROWS:(t + 1) * ROWS, :].T
        st[t]['thr'] = shard - 1 - ((y_row // BLOCK + t * (ROWS // BLOCK)) < jres).astype(jnp.int32)

    def score_steps(t):
        s = st[t]

        def local(start, size):
            def run():
                sc = jnp.dot(ext_rows(k_ext, t * ROWS + start, size), s['q_t'], preferred_element_type=F32)
                for off in range(0, size, BLOCK):
                    x0 = start + off
                    sub = sc[off:off + BLOCK]
                    if x0 < HALO:
                        seen = t * ROWS + x0 >= HALO - seq_loc * shard
                        sub = sub + jnp.where(seen, 0.0, neg).astype(F32)
                    if x0 < ROWS - BLOCK:
                        sub = jnp.where(y_row < x0 + BLOCK, sub, neg)
                    if x0 >= HALO:
                        col = lax.broadcasted_iota(jnp.int32, (BLOCK, ROWS), 0)
                        row = lax.broadcasted_iota(jnp.int32, (BLOCK, ROWS), 1)
                        sub = jnp.where(col + (x0 - HALO) <= row, sub, neg)
                    e_loc[t, x0:x0 + BLOCK, :] = sub
                    part = fold(sub, jnp.max)
                    s['mx'] = part if 'mx' not in s else jnp.maximum(s['mx'], part)
            return run

        def strided(start, size):
            def run():
                sc = jnp.dot(str_rows(ks_ref, start, size), s['q_t'], preferred_element_type=F32)
                for off in range(0, size, BLOCK):
                    x0 = start + off
                    sub = sc[off:off + BLOCK] + jnp.where(x0 // BLOCK < s['thr'], 0.0, neg).astype(F32)
                    e_str[t, x0:x0 + BLOCK, :] = sub
                    s['mx'] = jnp.maximum(s['mx'], fold(sub, jnp.max))
            return run

        def finish():
            s['m'] = jnp.max(s['mx'], axis=0, keepdims=True)
        return [local(*p) for p in pieces(win)] + [strided(*p) for p in pieces(n_str)] + [finish]

    def exp_steps(t):
        s = st[t]

        def one(ref, start, size):
            def run():
                e = jnp.exp2((ref[t, start:start + size, :] - s['m']) * to_exp2)
                ref[t, start:start + size, :] = e
                part = fold(e, jnp.sum)
                s['l'] = part if 'l' not in s else s['l'] + part
            return run

        def finish():
            s['inv'] = 1.0 / jnp.sum(s['l'], axis=0, keepdims=True)
        return [one(e_loc, *p) for p in pieces(win)] + [one(e_str, *p) for p in pieces(n_str)] + [finish]

    def out_steps(t):
        s = st[t]

        def loc(start, size):
            def run():
                pb_loc[t, start:start + size, :] = (e_loc[t, start:start + size, :] * s['inv']).astype(BF16)
            return run

        def strided(start, size):
            def run():
                pb_str[start:start + size, t * ROWS:(t + 1) * ROWS] = (e_str[t, start:start + size, :] * s['inv']).astype(BF16)
            return run

        def finish():
            o_t = (jnp.dot(v_t[:, t * ROWS:t * ROWS + win_pad], pb_loc[t], preferred_element_type=F32)
                   + jnp.dot(vs_t[...], pb_str[:, t * ROWS:(t + 1) * ROWS], preferred_element_type=F32))
            s['delta'] = jnp.sum(s['do_t'].astype(F32) * o_t, axis=0, keepdims=True)
            o_ref[0, 0, t * ROWS:(t + 1) * ROWS, :] = o_t.T.astype(BF16)
        return [loc(*p) for p in pieces(win)] + [strided(*p) for p in pieces(n_str)] + [finish]

    def grad_steps(t):
        s = st[t]

        def loc(start, size):
            def run():
                dp = jnp.dot(ext_rows(v_ext, t * ROWS + start, size), s['do_t'], preferred_element_type=F32)
                p = e_loc[t, start:start + size, :] * s['inv']
                ds_loc[t, start:start + size, :] = (p * (dp - s['delta'])).astype(BF16)
            return run

        def strided(start, size):
            def run():
                dp = jnp.dot(str_rows(vs_ref, start, size), s['do_t'], preferred_element_type=F32)
                p = e_str[t, start:start + size, :] * s['inv']
                ds_str[start:start + size, t * ROWS:(t + 1) * ROWS] = (p * (dp - s['delta'])).astype(BF16)
            return run
        return [loc(*p) for p in pieces(win)] + [strided(*p) for p in pieces(n_str)]

    def back_steps(t):
        def dv():
            dv_acc[BLOCK + t * ROWS:BLOCK + t * ROWS + win, :] += jnp.dot(pb_loc[t, :win, :], do_ref[0, 0, t * ROWS:(t + 1) * ROWS, :], preferred_element_type=F32)

        def dk():
            dk_acc[BLOCK + t * ROWS:BLOCK + t * ROWS + win, :] += jnp.dot(ds_loc[t, :win, :], q_ref[0, 0, t * ROWS:(t + 1) * ROWS, :], preferred_element_type=F32)

        def dq():
            dq_t = (jnp.dot(k_t[:, t * ROWS:t * ROWS + win_pad], ds_loc[t], preferred_element_type=F32)
                    + jnp.dot(ks_t[...], ds_str[:, t * ROWS:(t + 1) * ROWS], preferred_element_type=F32))
            dq_ref[0, 0, t * ROWS:(t + 1) * ROWS, :] = (dq_t * scale).T.astype(BF16)
        return [dv, dk, dq]

    def weave(*lists):
        total = max(len(x) for x in lists)
        for i in range(total):
            for x in lists:
                for j in range(i * len(x) // total, (i + 1) * len(x) // total):
                    x[j]()

    weave(score_steps(0))
    for t in range(n_tiles):
        later = score_steps(t + 1) if t + 1 < n_tiles else []
        earlier = back_steps(t - 1) if t > 0 else []
        weave(*[x for x in (exp_steps(t), later, earlier) if x])
        weave(out_steps(t))
        weave(grad_steps(t))
    weave(back_steps(n_tiles - 1))

    str_ref[:n_blk, 1, 0, member] = jnp.dot(pb_str[...], do_ref[0, 0], preferred_element_type=F32).reshape(n_blk, BLOCK, head_dim)
    dks = jnp.dot(ds_str[...], q_ref[0, 0], preferred_element_type=F32) * scale
    str_ref[:n_blk, 0, 0, member] = dks.reshape(n_blk, BLOCK, head_dim)

    @pl.when(member == group_size - 1)
    def _():
        near_dev = jnp.maximum(shard - 1, 0)
        far_dev = jnp.maximum(shard - 2, 0)
        for w, acc, factor in ((0, dk_acc, scale), (1, dv_acc, 1.0)):
            for slot in range(n_res):
                res = res_of(slot)
                far = acc[rows_at(res), :] * factor
                near = acc[rows_at(res + n_res), :] * factor
                own_ref[w, 0, slot] = acc[rows_at(res + 2 * n_res), :] * factor
                if slot < group_size:
                    str_ref[far_dev, w, 0, slot] += far
                    str_ref[near_dev, w, 0, slot] += near
                else:
                    rest2_ref[w, 0, slot - group_size] = far.astype(BF16)
                    rest1_ref[w, 0, slot - group_size] = near.astype(BF16)


def attention(first_head, n_heads, shard, q, d_out, kv_rot, rest1, rest2, gathered):
    _, group_size, seq_loc, head_dim = q.shape
    n_res = seq_loc // BLOCK
    n_rest = n_res - group_size
    cp_size = gathered.shape[0]
    n_blk = cp_size - 2
    n_str = n_blk * BLOCK
    win = HALO + ROWS
    win_pad = -(-win // 256) * 256
    n_tiles = seq_loc // ROWS
    ext_len = BLOCK + HALO + seq_loc
    ext_pad = (n_tiles - 1) * ROWS + win_pad
    spec_q = pl.BlockSpec((1, 1, seq_loc, head_dim), lambda g, u, s: (s[0] + g, u, 0, 0))
    spec_o = pl.BlockSpec((1, 1, seq_loc, head_dim), lambda g, u, s: (g, u, 0, 0))
    own = [pl.BlockSpec((1, 1, n_res, BLOCK, head_dim), lambda g, u, s, w=w: (w, g, 0, 0, 0)) for w in range(2)]
    prev = [[pl.BlockSpec((1, 1, 1, group_size, BLOCK, head_dim), lambda g, u, s, w=w, d=d: (jnp.maximum(s[1] - d, 0), w, g, 0, 0, 0)) for w in range(2)] for d in (1, 2)]
    rest = [pl.BlockSpec((1, 1, n_rest, BLOCK, head_dim), lambda g, u, s, w=w: (w, g, 0, 0, 0)) for w in range(2)]
    strided = [pl.BlockSpec((n_blk, 1, 1, 1, BLOCK, head_dim), lambda g, u, s, w=w: (0, w, g, u, 0, 0)) for w in range(2)]
    spec_own = pl.BlockSpec((2, 1, n_res, BLOCK, head_dim), lambda g, u, s: (0, g, 0, 0, 0))
    spec_rest = pl.BlockSpec((2, 1, n_rest, BLOCK, head_dim), lambda g, u, s: (0, g, 0, 0, 0))
    spec_str = pl.BlockSpec((cp_size, 2, 1, group_size, BLOCK, head_dim), lambda g, u, s: (0, 0, g, 0, 0, 0))
    sds = jax.ShapeDtypeStruct
    flops = n_heads * group_size * 6 * 2 * seq_loc * (win + n_str) * head_dim
    info = jnp.stack([jnp.int32(first_head), shard.astype(jnp.int32)])
    return pl.pallas_call(
        attention_kernel,
        grid_spec=pltpu.PrefetchScalarGridSpec(
            num_scalar_prefetch=1,
            grid=(n_heads, group_size),
            in_specs=[spec_q, spec_q, *own, *prev[0], *prev[1], *rest, *rest, *strided],
            out_specs=[spec_o, spec_o, spec_own, spec_rest, spec_rest, spec_str],
            scratch_shapes=[
                pltpu.VMEM((ext_len, head_dim), BF16), pltpu.VMEM((ext_len, head_dim), BF16),
                pltpu.VMEM((head_dim, ext_pad), BF16), pltpu.VMEM((head_dim, ext_pad), BF16),
                pltpu.VMEM((head_dim, n_str), BF16), pltpu.VMEM((head_dim, n_str), BF16),
                pltpu.VMEM((ext_len, head_dim), F32), pltpu.VMEM((ext_len, head_dim), F32),
                pltpu.VMEM((n_tiles, win, ROWS), F32), pltpu.VMEM((n_tiles, n_str, ROWS), F32),
                pltpu.VMEM((n_tiles, win_pad, ROWS), BF16), pltpu.VMEM((n_str, seq_loc), BF16),
                pltpu.VMEM((n_tiles, win_pad, ROWS), BF16), pltpu.VMEM((n_str, seq_loc), BF16),
            ]),
        out_shape=[
            sds((n_heads, group_size, seq_loc, head_dim), BF16), sds((n_heads, group_size, seq_loc, head_dim), BF16),
            sds((2, n_heads, n_res, BLOCK, head_dim), F32),
            sds((2, n_heads, n_rest, BLOCK, head_dim), BF16), sds((2, n_heads, n_rest, BLOCK, head_dim), BF16),
            sds((cp_size, 2, n_heads, group_size, BLOCK, head_dim), F32),
        ],
        compiler_params=pltpu.CompilerParams(vmem_limit_bytes=56 * 1024 * 1024),
        cost_estimate=pl.CostEstimate(flops=flops, bytes_accessed=0, transcendentals=0),
        name='attention',
    )(info, q, d_out, kv_rot, kv_rot, gathered, gathered, gathered, gathered, rest1, rest1, rest2, rest2, gathered, gathered)


def rotate_kernel(first_head, group_size, k_ref, v_ref, out_ref):
    n_res = out_ref.shape[2]
    for w, ref in enumerate((k_ref, v_ref)):
        for slot in range(n_res):
            res = lax.rem(STRIDE * 64 - 1 - ((first_head + pl.program_id(0)) * group_size + slot), STRIDE)
            out_ref[w, 0, slot] = ref[0, pl.ds(pl.multiple_of(res * BLOCK, BLOCK), BLOCK), :]


def rotate(first_head, n_heads, k_h, v_h, group_size):
    _, seq_loc, head_dim = k_h.shape
    n_res = seq_loc // BLOCK
    spec = pl.BlockSpec((1, seq_loc, head_dim), lambda g: (first_head + g, 0, 0))
    return pl.pallas_call(
        functools.partial(rotate_kernel, first_head, group_size),
        grid=(n_heads,),
        in_specs=[spec, spec],
        out_specs=pl.BlockSpec((2, 1, n_res, BLOCK, head_dim), lambda g: (0, g, 0, 0, 0)),
        out_shape=jax.ShapeDtypeStruct((2, n_heads, n_res, BLOCK, head_dim), BF16),
        cost_estimate=pl.CostEstimate(flops=10 ** 7, bytes_accessed=0, transcendentals=0),
        name='rotate',
    )(k_h, v_h)


def merge_kernel(first_head, own_ref, red_ref, back1_ref, back2_ref, out_ref):
    n_res, group_size = own_ref.shape[2], red_ref.shape[2]
    for w in range(2):
        for slot in range(n_res):
            res = lax.rem(STRIDE * 64 - 1 - ((first_head + pl.program_id(0)) * group_size + slot), STRIDE)
            if slot < group_size:
                total = own_ref[w, 0, slot] + red_ref[w, 0, slot]
            else:
                total = own_ref[w, 0, slot] + back1_ref[w, 0, slot - group_size].astype(F32) + back2_ref[w, 0, slot - group_size].astype(F32)
            out_ref[w, 0, pl.ds(pl.multiple_of(res * BLOCK, BLOCK), BLOCK), :] = total.astype(BF16)


def merge(first_head, own, reduced, back1, back2):
    _, n_heads, n_res, _, head_dim = own.shape
    group_size, n_rest = reduced.shape[2], back1.shape[2]
    seq_loc = n_res * BLOCK

    def spec(count):
        return pl.BlockSpec((2, 1, count, BLOCK, head_dim), lambda g: (0, g, 0, 0, 0))
    return pl.pallas_call(
        functools.partial(merge_kernel, first_head),
        grid=(n_heads,),
        in_specs=[spec(n_res), spec(group_size), spec(n_rest), spec(n_rest)],
        out_specs=pl.BlockSpec((2, 1, seq_loc, head_dim), lambda g: (0, g, 0, 0)),
        out_shape=jax.ShapeDtypeStruct((2, n_heads, seq_loc, head_dim), BF16),
        cost_estimate=pl.CostEstimate(flops=10 ** 7, bytes_accessed=0, transcendentals=0),
        name='merge',
    )(own, reduced, back1, back2)


def solution(mesh):
    cp_size = mesh.shape['cp']
    spec = P('dp', 'cp', None, None)

    def per_device(q_rope, k_rope, values, d_out):
        seq_loc, heads, head_dim = q_rope.shape[1:]
        kv_heads = k_rope.shape[2]
        group_size = heads // kv_heads
        shard = lax.axis_index('cp')
        starts = [sum(CHUNKS[:i]) for i in range(len(CHUNKS))]
        k_h, v_h = jnp.swapaxes(k_rope[0], 0, 1), jnp.swapaxes(values[0], 0, 1)

        def onward(x):
            return lax.ppermute(x, 'cp', [(s, s + 1) for s in range(cp_size - 1)])

        kv_rot = [rotate(a, n, k_h, v_h, group_size) for a, n in zip(starts, CHUNKS)]
        gathered = [lax.all_gather(x[:, :, :group_size], 'cp', axis=0, tiled=False) for x in kv_rot]
        rest1 = [onward(x[:, :, group_size:]) for x in kv_rot]
        rest2 = [onward(x) for x in rest1]

        def head_major(x):
            return jnp.transpose(x[0].reshape(seq_loc, kv_heads, group_size, head_dim), (1, 2, 0, 3))

        q_h, do_h = head_major(q_rope), head_major(d_out)
        outs = [attention(a, n, shard, q_h, do_h, kv_rot[i], rest1[i], rest2[i], gathered[i]) for i, (a, n) in enumerate(zip(starts, CHUNKS))]
        reduced = [lax.psum_scatter(out[5], 'cp', scatter_dimension=0, tiled=False) for out in outs]

        def token_major(xs):
            x = jnp.concatenate(xs, axis=0)
            return jnp.transpose(x, (2, 0, 1, 3)).reshape(1, seq_loc, heads, head_dim)

        attn_out = token_major([out[0] for out in outs])
        d_q = token_major([out[1] for out in outs])

        merged = []
        for i, (out, red) in enumerate(zip(outs, reduced)):
            back = [lax.ppermute(out[2 + dist], 'cp', [(s + dist, s) for s in range(cp_size - dist)]) for dist in (1, 2)]
            merged.append(merge(starts[i], out[2], red, back[0], back[1]))
        plain = jnp.swapaxes(jnp.concatenate(merged, axis=1), 1, 2)
        return attn_out, d_q, plain[0][None], plain[1][None]

    return jax.shard_map(per_device, mesh=mesh, in_specs=(spec, spec, spec, spec), out_specs=(spec, spec, spec, spec), check_vma=False)
```

```python
import functools

import jax
import jax.numpy as jnp
from jax import lax
from jax.experimental import pallas as pl
from jax.experimental.pallas import tpu as pltpu
from jax.sharding import PartitionSpec as P

BLOCK = 64
LOCAL = 16
STRIDE = 8
HALO = (LOCAL - 1) * BLOCK
ROWS = 256
CHUNK = 128
LOG2E = 1.4426950408889634
CHUNKS = (3, 3, 2)
F32 = jnp.float32
BF16 = jnp.bfloat16


def fold(x, op):
    rows, cols = x.shape
    return op(x.reshape(rows // 8, 8, cols), axis=0)


def pieces(total):
    return [(start, min(CHUNK, total - start)) for start in range(0, total, CHUNK)]


def attention_kernel(info_ref, q_ref, do_ref, ko_ref, vo_ref, k1_ref, v1_ref, k2_ref, v2_ref, kr1_ref, vr1_ref, kr2_ref, vr2_ref, ks_ref, vs_ref,
                     o_ref, dq_ref, own_ref, rest1_ref, rest2_ref, str_ref,
                     k_ext, v_ext, k_t, v_t, ks_t, vs_t, dk_acc, dv_acc, e_loc, e_str, pb_loc, pb_str, ds_loc, ds_str):
    shard = info_ref[1]
    head_idx, member = pl.program_id(0), pl.program_id(1)
    group_size = str_ref.shape[3]
    seq_loc, head_dim = q_ref.shape[2], q_ref.shape[3]
    n_res = seq_loc // BLOCK
    n_tiles = seq_loc // ROWS
    win = HALO + ROWS
    win_pad = pb_loc.shape[1]
    n_str = ks_t.shape[1]
    n_blk = n_str // BLOCK
    scale = 1.0 / head_dim
    to_exp2 = scale * LOG2E
    neg = -jnp.inf

    def res_of(slot):
        return lax.rem(STRIDE * 64 - 1 - ((info_ref[0] + head_idx) * group_size + slot), STRIDE)

    def rows_at(block):
        return pl.ds(pl.multiple_of(block * BLOCK, BLOCK), BLOCK)

    jres = res_of(member)

    @pl.when((head_idx == 0) & (member == 0))
    def _():
        for t in range(n_tiles):
            pb_loc[t, win:, :] = jnp.zeros((win_pad - win, ROWS), BF16)
            ds_loc[t, win:, :] = jnp.zeros((win_pad - win, ROWS), BF16)

    @pl.when(member == 0)
    def _():
        for ext, own, near, far, near_rest, far_rest in ((k_ext, ko_ref, k1_ref, k2_ref, kr1_ref, kr2_ref), (v_ext, vo_ref, v1_ref, v2_ref, vr1_ref, vr2_ref)):
            for slot in range(n_res):
                res = res_of(slot)
                far_blk = far[0, 0, 0, slot] if slot < group_size else far_rest[0, 0, slot - group_size]
                near_blk = near[0, 0, 0, slot] if slot < group_size else near_rest[0, 0, slot - group_size]
                ext[rows_at(res), :] = far_blk
                ext[rows_at(res + n_res), :] = near_blk
                ext[rows_at(res + 2 * n_res), :] = own[0, 0, slot]
        k_t[...] = jnp.zeros_like(k_t)
        v_t[...] = jnp.zeros_like(v_t)
        k_t[:, :HALO + seq_loc] = k_ext[BLOCK:, :].T
        v_t[:, :HALO + seq_loc] = v_ext[BLOCK:, :].T
        dk_acc[...] = jnp.zeros_like(dk_acc)
        dv_acc[...] = jnp.zeros_like(dv_acc)
        str_ref[n_blk:] = jnp.zeros((str_ref.shape[0] - n_blk,) + str_ref.shape[1:], F32)

    def str_rows(ref, start, size):
        return ref[start // BLOCK:(start + size) // BLOCK, 0, 0, 0].reshape(size, head_dim)

    def ext_rows(ref, start, size):
        return ref[BLOCK + start:BLOCK + start + size, :]

    ks_t[...] = str_rows(ks_ref, 0, n_str).T
    vs_t[...] = str_rows(vs_ref, 0, n_str).T

    y_row = lax.broadcasted_iota(jnp.int32, (1, ROWS), 1)
    st = [dict() for _ in range(n_tiles)]
    for t in range(n_tiles):
        st[t]['q_t'] = q_ref[0, 0, t * ROWS:(t + 1) * ROWS, :].T
        st[t]['do_t'] = do_ref[0, 0, t * ROWS:(t + 1) * ROWS, :].T
        st[t]['thr'] = shard - 1 - ((y_row // BLOCK + t * (ROWS // BLOCK)) < jres).astype(jnp.int32)

    def score_steps(t):
        s = st[t]

        def local(start, size):
            def run():
                sc = jnp.dot(ext_rows(k_ext, t * ROWS + start, size), s['q_t'], preferred_element_type=F32)
                for off in range(0, size, BLOCK):
                    x0 = start + off
                    sub = sc[off:off + BLOCK]
                    if x0 < HALO:
                        seen = t * ROWS + x0 >= HALO - seq_loc * shard
                        sub = sub + jnp.where(seen, 0.0, neg).astype(F32)
                    if x0 < ROWS - BLOCK:
                        sub = jnp.where(y_row < x0 + BLOCK, sub, neg)
                    if x0 >= HALO:
                        col = lax.broadcasted_iota(jnp.int32, (BLOCK, ROWS), 0)
                        row = lax.broadcasted_iota(jnp.int32, (BLOCK, ROWS), 1)
                        sub = jnp.where(col + (x0 - HALO) <= row, sub, neg)
                    e_loc[t, x0:x0 + BLOCK, :] = sub
                    part = fold(sub, jnp.max)
                    s['mx'] = part if 'mx' not in s else jnp.maximum(s['mx'], part)
            return run

        def strided(start, size):
            def run():
                sc = jnp.dot(str_rows(ks_ref, start, size), s['q_t'], preferred_element_type=F32)
                for off in range(0, size, BLOCK):
                    x0 = start + off
                    sub = sc[off:off + BLOCK] + jnp.where(x0 // BLOCK < s['thr'], 0.0, neg).astype(F32)
                    e_str[t, x0:x0 + BLOCK, :] = sub
                    s['mx'] = jnp.maximum(s['mx'], fold(sub, jnp.max))
            return run

        def finish():
            s['m'] = jnp.max(s['mx'], axis=0, keepdims=True)
        return [local(*p) for p in pieces(win)] + [strided(*p) for p in pieces(n_str)] + [finish]

    def exp_steps(t):
        s = st[t]

        def one(ref, start, size):
            def run():
                e = jnp.exp2((ref[t, start:start + size, :] - s['m']) * to_exp2)
                ref[t, start:start + size, :] = e
                part = fold(e, jnp.sum)
                s['l'] = part if 'l' not in s else s['l'] + part
            return run

        def finish():
            s['inv'] = 1.0 / jnp.sum(s['l'], axis=0, keepdims=True)
        return [one(e_loc, *p) for p in pieces(win)] + [one(e_str, *p) for p in pieces(n_str)] + [finish]

    def out_steps(t):
        s = st[t]

        def loc(start, size):
            def run():
                pb_loc[t, start:start + size, :] = (e_loc[t, start:start + size, :] * s['inv']).astype(BF16)
            return run

        def strided(start, size):
            def run():
                pb_str[start:start + size, t * ROWS:(t + 1) * ROWS] = (e_str[t, start:start + size, :] * s['inv']).astype(BF16)
            return run

        def finish():
            o_t = (jnp.dot(v_t[:, t * ROWS:t * ROWS + win_pad], pb_loc[t], preferred_element_type=F32)
                   + jnp.dot(vs_t[...], pb_str[:, t * ROWS:(t + 1) * ROWS], preferred_element_type=F32))
            s['delta'] = jnp.sum(s['do_t'].astype(F32) * o_t, axis=0, keepdims=True)
            o_ref[0, 0, t * ROWS:(t + 1) * ROWS, :] = o_t.T.astype(BF16)
        return [loc(*p) for p in pieces(win)] + [strided(*p) for p in pieces(n_str)] + [finish]

    def grad_steps(t):
        s = st[t]

        def loc(start, size):
            def run():
                dp = jnp.dot(ext_rows(v_ext, t * ROWS + start, size), s['do_t'], preferred_element_type=F32)
                p = e_loc[t, start:start + size, :] * s['inv']
                ds_loc[t, start:start + size, :] = (p * (dp - s['delta'])).astype(BF16)
            return run

        def strided(start, size):
            def run():
                dp = jnp.dot(str_rows(vs_ref, start, size), s['do_t'], preferred_element_type=F32)
                p = e_str[t, start:start + size, :] * s['inv']
                ds_str[start:start + size, t * ROWS:(t + 1) * ROWS] = (p * (dp - s['delta'])).astype(BF16)
            return run
        return [loc(*p) for p in pieces(win)] + [strided(*p) for p in pieces(n_str)]

    def back_steps(t):
        def dv():
            dv_acc[BLOCK + t * ROWS:BLOCK + t * ROWS + win, :] += jnp.dot(pb_loc[t, :win, :], do_ref[0, 0, t * ROWS:(t + 1) * ROWS, :], preferred_element_type=F32)

        def dk():
            dk_acc[BLOCK + t * ROWS:BLOCK + t * ROWS + win, :] += jnp.dot(ds_loc[t, :win, :], q_ref[0, 0, t * ROWS:(t + 1) * ROWS, :], preferred_element_type=F32)

        def dq():
            dq_t = (jnp.dot(k_t[:, t * ROWS:t * ROWS + win_pad], ds_loc[t], preferred_element_type=F32)
                    + jnp.dot(ks_t[...], ds_str[:, t * ROWS:(t + 1) * ROWS], preferred_element_type=F32))
            dq_ref[0, 0, t * ROWS:(t + 1) * ROWS, :] = (dq_t * scale).T.astype(BF16)
        return [dv, dk, dq]

    def weave(*lists):
        total = max(len(x) for x in lists)
        for i in range(total):
            for x in lists:
                for j in range(i * len(x) // total, (i + 1) * len(x) // total):
                    x[j]()

    weave(score_steps(0))
    for t in range(n_tiles):
        later = score_steps(t + 1) if t + 1 < n_tiles else []
        earlier = back_steps(t - 1) if t > 0 else []
        weave(*[x for x in (exp_steps(t), later, earlier) if x])
        weave(out_steps(t))
        weave(grad_steps(t))
    weave(back_steps(n_tiles - 1))

    str_ref[:n_blk, 1, 0, member] = jnp.dot(pb_str[...], do_ref[0, 0], preferred_element_type=F32).reshape(n_blk, BLOCK, head_dim)
    dks = jnp.dot(ds_str[...], q_ref[0, 0], preferred_element_type=F32) * scale
    str_ref[:n_blk, 0, 0, member] = dks.reshape(n_blk, BLOCK, head_dim)

    @pl.when(member == group_size - 1)
    def _():
        near_dev = jnp.maximum(shard - 1, 0)
        far_dev = jnp.maximum(shard - 2, 0)
        for w, acc, factor in ((0, dk_acc, scale), (1, dv_acc, 1.0)):
            for slot in range(n_res):
                res = res_of(slot)
                far = acc[rows_at(res), :] * factor
                near = acc[rows_at(res + n_res), :] * factor
                own_ref[w, 0, slot] = acc[rows_at(res + 2 * n_res), :] * factor
                if slot < group_size:
                    str_ref[far_dev, w, 0, slot] += far
                    str_ref[near_dev, w, 0, slot] += near
                else:
                    rest2_ref[w, 0, slot - group_size] = far.astype(BF16)
                    rest1_ref[w, 0, slot - group_size] = near.astype(BF16)


def attention(first_head, n_heads, shard, q, d_out, kv_rot, rest1, rest2, gathered):
    _, group_size, seq_loc, head_dim = q.shape
    n_res = seq_loc // BLOCK
    n_rest = n_res - group_size
    cp_size = gathered.shape[0]
    n_blk = cp_size - 2
    n_str = n_blk * BLOCK
    win = HALO + ROWS
    win_pad = -(-win // 256) * 256
    n_tiles = seq_loc // ROWS
    ext_len = BLOCK + HALO + seq_loc
    ext_pad = (n_tiles - 1) * ROWS + win_pad
    spec_q = pl.BlockSpec((1, 1, seq_loc, head_dim), lambda g, u, s: (s[0] + g, u, 0, 0))
    spec_o = pl.BlockSpec((1, 1, seq_loc, head_dim), lambda g, u, s: (g, u, 0, 0))
    own = [pl.BlockSpec((1, 1, n_res, BLOCK, head_dim), lambda g, u, s, w=w: (w, g, 0, 0, 0)) for w in range(2)]
    prev = [[pl.BlockSpec((1, 1, 1, group_size, BLOCK, head_dim), lambda g, u, s, w=w, d=d: (jnp.maximum(s[1] - d, 0), w, g, 0, 0, 0)) for w in range(2)] for d in (1, 2)]
    rest = [pl.BlockSpec((1, 1, n_rest, BLOCK, head_dim), lambda g, u, s, w=w: (w, g, 0, 0, 0)) for w in range(2)]
    strided = [pl.BlockSpec((n_blk, 1, 1, 1, BLOCK, head_dim), lambda g, u, s, w=w: (0, w, g, u, 0, 0)) for w in range(2)]
    spec_own = pl.BlockSpec((2, 1, n_res, BLOCK, head_dim), lambda g, u, s: (0, g, 0, 0, 0))
    spec_rest = pl.BlockSpec((2, 1, n_rest, BLOCK, head_dim), lambda g, u, s: (0, g, 0, 0, 0))
    spec_str = pl.BlockSpec((cp_size, 2, 1, group_size, BLOCK, head_dim), lambda g, u, s: (0, 0, g, 0, 0, 0))
    sds = jax.ShapeDtypeStruct
    flops = n_heads * group_size * 6 * 2 * seq_loc * (win + n_str) * head_dim
    info = jnp.stack([jnp.int32(first_head), shard.astype(jnp.int32)])
    return pl.pallas_call(
        attention_kernel,
        grid_spec=pltpu.PrefetchScalarGridSpec(
            num_scalar_prefetch=1,
            grid=(n_heads, group_size),
            in_specs=[spec_q, spec_q, *own, *prev[0], *prev[1], *rest, *rest, *strided],
            out_specs=[spec_o, spec_o, spec_own, spec_rest, spec_rest, spec_str],
            scratch_shapes=[
                pltpu.VMEM((ext_len, head_dim), BF16), pltpu.VMEM((ext_len, head_dim), BF16),
                pltpu.VMEM((head_dim, ext_pad), BF16), pltpu.VMEM((head_dim, ext_pad), BF16),
                pltpu.VMEM((head_dim, n_str), BF16), pltpu.VMEM((head_dim, n_str), BF16),
                pltpu.VMEM((ext_len, head_dim), F32), pltpu.VMEM((ext_len, head_dim), F32),
                pltpu.VMEM((n_tiles, win, ROWS), F32), pltpu.VMEM((n_tiles, n_str, ROWS), F32),
                pltpu.VMEM((n_tiles, win_pad, ROWS), BF16), pltpu.VMEM((n_str, seq_loc), BF16),
                pltpu.VMEM((n_tiles, win_pad, ROWS), BF16), pltpu.VMEM((n_str, seq_loc), BF16),
            ]),
        out_shape=[
            sds((n_heads, group_size, seq_loc, head_dim), BF16), sds((n_heads, group_size, seq_loc, head_dim), BF16),
            sds((2, n_heads, n_res, BLOCK, head_dim), F32),
            sds((2, n_heads, n_rest, BLOCK, head_dim), BF16), sds((2, n_heads, n_rest, BLOCK, head_dim), BF16),
            sds((cp_size, 2, n_heads, group_size, BLOCK, head_dim), F32),
        ],
        compiler_params=pltpu.CompilerParams(vmem_limit_bytes=56 * 1024 * 1024),
        cost_estimate=pl.CostEstimate(flops=flops, bytes_accessed=0, transcendentals=0),
        name='attention',
    )(info, q, d_out, kv_rot, kv_rot, gathered, gathered, gathered, gathered, rest1, rest1, rest2, rest2, gathered, gathered)


def rotate_kernel(first_head, group_size, k_ref, v_ref, out_ref):
    n_res = out_ref.shape[2]
    for w, ref in enumerate((k_ref, v_ref)):
        for slot in range(n_res):
            res = lax.rem(STRIDE * 64 - 1 - ((first_head + pl.program_id(0)) * group_size + slot), STRIDE)
            out_ref[w, 0, slot] = ref[0, pl.ds(pl.multiple_of(res * BLOCK, BLOCK), BLOCK), :]


def rotate(first_head, n_heads, k_h, v_h, group_size):
    _, seq_loc, head_dim = k_h.shape
    n_res = seq_loc // BLOCK
    spec = pl.BlockSpec((1, seq_loc, head_dim), lambda g: (first_head + g, 0, 0))
    return pl.pallas_call(
        functools.partial(rotate_kernel, first_head, group_size),
        grid=(n_heads,),
        in_specs=[spec, spec],
        out_specs=pl.BlockSpec((2, 1, n_res, BLOCK, head_dim), lambda g: (0, g, 0, 0, 0)),
        out_shape=jax.ShapeDtypeStruct((2, n_heads, n_res, BLOCK, head_dim), BF16),
        cost_estimate=pl.CostEstimate(flops=10 ** 7, bytes_accessed=0, transcendentals=0),
        name='rotate',
    )(k_h, v_h)


def merge_kernel(first_head, own_ref, red_ref, back1_ref, back2_ref, out_ref):
    n_res, group_size = own_ref.shape[2], red_ref.shape[2]
    for w in range(2):
        for slot in range(n_res):
            res = lax.rem(STRIDE * 64 - 1 - ((first_head + pl.program_id(0)) * group_size + slot), STRIDE)
            if slot < group_size:
                total = own_ref[w, 0, slot] + red_ref[w, 0, slot]
            else:
                total = own_ref[w, 0, slot] + back1_ref[w, 0, slot - group_size].astype(F32) + back2_ref[w, 0, slot - group_size].astype(F32)
            out_ref[w, 0, pl.ds(pl.multiple_of(res * BLOCK, BLOCK), BLOCK), :] = total.astype(BF16)


def merge(first_head, own, reduced, back1, back2):
    _, n_heads, n_res, _, head_dim = own.shape
    group_size, n_rest = reduced.shape[2], back1.shape[2]
    seq_loc = n_res * BLOCK

    def spec(count):
        return pl.BlockSpec((2, 1, count, BLOCK, head_dim), lambda g: (0, g, 0, 0, 0))
    return pl.pallas_call(
        functools.partial(merge_kernel, first_head),
        grid=(n_heads,),
        in_specs=[spec(n_res), spec(group_size), spec(n_rest), spec(n_rest)],
        out_specs=pl.BlockSpec((2, 1, seq_loc, head_dim), lambda g: (0, g, 0, 0)),
        out_shape=jax.ShapeDtypeStruct((2, n_heads, seq_loc, head_dim), BF16),
        cost_estimate=pl.CostEstimate(flops=10 ** 7, bytes_accessed=0, transcendentals=0),
        name='merge',
    )(own, reduced, back1, back2)


def solution(mesh):
    cp_size = mesh.shape['cp']
    spec = P('dp', 'cp', None, None)

    def per_device(q_rope, k_rope, values, d_out):
        seq_loc, heads, head_dim = q_rope.shape[1:]
        kv_heads = k_rope.shape[2]
        group_size = heads // kv_heads
        shard = lax.axis_index('cp')
        starts = [sum(CHUNKS[:i]) for i in range(len(CHUNKS))]
        k_h, v_h = jnp.swapaxes(k_rope[0], 0, 1), jnp.swapaxes(values[0], 0, 1)

        def onward(x):
            return lax.ppermute(x, 'cp', [(s, s + 1) for s in range(cp_size - 1)])

        kv_rot = [rotate(a, n, k_h, v_h, group_size) for a, n in zip(starts, CHUNKS)]
        gathered = [lax.all_gather(x[:, :, :group_size], 'cp', axis=0, tiled=False) for x in kv_rot]
        rest1 = [onward(x[:, :, group_size:]) for x in kv_rot]
        rest2 = [onward(x) for x in rest1]

        def head_major(x):
            return jnp.transpose(x[0].reshape(seq_loc, kv_heads, group_size, head_dim), (1, 2, 0, 3))

        q_h, do_h = head_major(q_rope), head_major(d_out)
        outs = [attention(a, n, shard, q_h, do_h, kv_rot[i], rest1[i], rest2[i], gathered[i]) for i, (a, n) in enumerate(zip(starts, CHUNKS))]
        reduced = [lax.psum_scatter(out[5], 'cp', scatter_dimension=0, tiled=False) for out in outs]

        def token_major(xs):
            x = jnp.concatenate(xs, axis=0)
            return jnp.transpose(x, (2, 0, 1, 3)).reshape(1, seq_loc, heads, head_dim)

        attn_out = token_major([out[0] for out in outs])
        d_q = token_major([out[1] for out in outs])

        merged = []
        for i, (out, red) in enumerate(zip(outs, reduced)):
            back = [lax.ppermute(out[2 + dist], 'cp', [(s + dist, s) for s in range(cp_size - dist)]) for dist in (1, 2)]
            merged.append(merge(starts[i], out[2], red, back[0], back[1]))
        plain = jnp.swapaxes(jnp.concatenate(merged, axis=1), 1, 2)
        return attn_out, d_q, plain[0][None], plain[1][None]

    return jax.shard_map(per_device, mesh=mesh, in_specs=(spec, spec, spec, spec), out_specs=(spec, spec, spec, spec), check_vma=False)
```
